16 devices in a mesh: outer: 2 (over z), inner: 8 (over y, x, core).
Axes of the slice: x: 2, y: 2, z: 2, core: 2. Of those that a mesh axis runs over, the one named last changes fastest.
Arguments:
- g_emb: float32 [16, 4096, 1024], P(('outer', 'inner'))
- g_qkv: float32 [16, 1, 1024, 3072], P(('outer', 'inner'))
- g_o: float32 [16, 1, 1024, 1024], P(('outer', 'inner'))
- g_w1: float32 [16, 1, 1024, 2816], P(('outer', 'inner'))
- g_w2: float32 [16, 1, 2816, 1024], P(('outer', 'inner'))
- g_bqkv: float32 [16, 1, 3072], P(('outer', 'inner'))
- g_b1: float32 [16, 1, 2816], P(('outer', 'inner'))
- g_dvec: float32 [16, 1, 6, 1024], P(('outer', 'inner'))
- m: float32 [14167808], P(('outer', 'inner'))
- v: float32 [14167808], P(('outer', 'inner'))
- w: float32 [14167808], P(('outer', 'inner'))
- lr: float32 [], replicated
- beta1: float32 [], replicated
- beta2: float32 [], replicated
- eps: float32 [], replicated
- step: int32 [], replicated
Outputs:
- output 1: float32 [14167808], P(('outer', 'inner'))
- output 2: float32 [14167808], P(('outer', 'inner'))
- output 3: float32 [14167808], P(('outer', 'inner'))
- output 4: bfloat16 [4096, 1024], replicated
- output 5: bfloat16 [1, 1024, 3072], replicated
- output 6: bfloat16 [1, 1024, 1024], replicated
- output 7: bfloat16 [1, 1024, 2816], replicated
- output 8: bfloat16 [1, 2816, 1024], replicated
- output 9: bfloat16 [1, 3072], replicated
- output 10: bfloat16 [1, 2816], replicated
- output 11: bfloat16 [1, 6, 1024], replicated
All inputs are finite; a program needn't handle non-finite values.
Results may differ from the reference program's by a relative error of at most 0.001.
Values are sent between devices in bfloat16 or wider.
A program may use at most 1 GiB of HBM per device.

```python
import math
import jax
import jax.numpy as jnp

DEVICES = 16
D = 1024
FF = 2816
LAYERS = 1
EMB_ROWS = 4096

SHAPES = (
    (EMB_ROWS, D),
    (LAYERS, D, 3 * D),
    (LAYERS, D, D),
    (LAYERS, D, FF),
    (LAYERS, FF, D),
    (LAYERS, 3 * D),
    (LAYERS, FF),
    (LAYERS, 6, D),
)
SIZES = tuple(math.prod(s) for s in SHAPES)
PSI = sum(SIZES)
NAMES = ("g_emb", "g_qkv", "g_o", "g_w1", "g_w2", "g_bqkv", "g_b1", "g_dvec")


def draw_grad(key, shape):
    k1, k2 = jax.random.split(key)
    common = jax.random.normal(k1, shape, jnp.float32)
    own = jax.random.normal(k2, (DEVICES,) + shape, jnp.float32)
    return common[None] + 4.0 * own


def setup_inputs(seed: int = 0) -> dict:
    ks = jax.random.split(jax.random.key(seed), 16)
    out = {}
    for i in range(8):
        out[NAMES[i]] = draw_grad(ks[i], SHAPES[i])
    out["m"] = jax.random.normal(ks[8], (PSI,), jnp.float32)
    out["v"] = jax.random.uniform(ks[9], (PSI,), jnp.float32, 1.0, 4.0)
    out["w"] = jax.random.normal(ks[10], (PSI,), jnp.float32)
    out["lr"] = jax.random.uniform(ks[11], (), jnp.float32, 0.12, 0.2)
    out["beta1"] = jax.random.uniform(ks[12], (), jnp.float32, 0.5, 0.7)
    out["beta2"] = jax.random.uniform(ks[13], (), jnp.float32, 0.7, 0.9)
    out["eps"] = jax.random.uniform(ks[14], (), jnp.float32, 0.1, 1.5)
    out["step"] = jax.random.randint(ks[15], (), 1, 6, jnp.int32)
    return out


def reference(g_emb, g_qkv, g_o, g_w1, g_w2, g_bqkv, g_b1, g_dvec, m, v, w, lr, beta1, beta2, eps, step):
    grads = (g_emb, g_qkv, g_o, g_w1, g_w2, g_bqkv, g_b1, g_dvec)
    g = jnp.concatenate([jnp.sum(x, axis=0).reshape(-1) for x in grads]) / DEVICES
    t = step.astype(jnp.float32)
    m_new = beta1 * m + (1.0 - beta1) * g
    v_new = beta2 * v + (1.0 - beta2) * (g * g)
    m_hat = m_new / (1.0 - beta1 ** t)
    v_hat = v_new / (1.0 - beta2 ** t)
    w_new = w - lr * m_hat / (jnp.sqrt(v_hat) + eps)
    flat = w_new.astype(jnp.bfloat16)
    wb = []
    start = 0
    for i in range(8):
        wb.append(flat[start:start + SIZES[i]].reshape(SHAPES[i]))
        start = start + SIZES[i]
    return (m_new, v_new, w_new, wb[0], wb[1], wb[2], wb[3], wb[4], wb[5], wb[6], wb[7])
```

```python
import functools
import math
import jax
import jax.numpy as jnp
from jax import lax
from jax.experimental import pallas as pl
from jax.experimental.pallas import tpu as pltpu
from jax.sharding import PartitionSpec as P

AXES = ("outer", "inner")
MESH = pl.DeviceIdType.MESH
F32, BF16 = jnp.float32, jnp.bfloat16
NDEV = 16
SHARD = 885488
BIG = ((4096, 1024), (1024, 3072), (1024, 1024), (1024, 2816), (2816, 1024))
PER = tuple(c // 128 for _, c in BIG) + (1,)
SMALL = (3072, 2816, 6144)
SMALL_TILES = 32
TOFF = [0]
for _r, _c in BIG:
    TOFF.append(TOFF[-1] + _r * _c // 1024)
TOFF.append(TOFF[-1] + SMALL_TILES)
NBLK = tuple((TOFF[k + 1] - TOFF[k]) // PER[k] for k in range(6))

WIN = 888
SUB = 148
CH = SUB * 8
WR = WIN * 8
PIECE = 4
COLORS = ((1, 2, 3), (2, 3, 1), (3, 1, 2))


def win_start(w):
    def ge(t):
        return (w + 16 - t) // 16
    return 864 * w + 8 * (ge(9) - ge(5) - ge(10) + 2 * ge(11) - ge(12) + ge(13))


def block_start(w):
    e = w * SHARD
    t = e // 1024
    k = max(i for i in range(6) if TOFF[i] <= t)
    n = PER[k]
    return TOFF[k] + ((e - TOFF[k] * 1024) // (n * 1024)) * n, n, k


def my_id():
    return lax.axis_index("outer") * 8 + lax.axis_index("inner")


def coords(d):
    return (d // 8, d % 8)


def deltas(me):
    return [(1 - 2 * ((me // (1 << d)) % 2)) * (1 << d) for d in range(4)]


def entry_barrier(peers):
    sem = pltpu.get_barrier_semaphore()
    for p in peers:
        pl.semaphore_signal(sem, inc=1, device_id=p, device_id_type=MESH)
    pl.semaphore_wait(sem, 4)


BLK = 4096
NB = SHARD // BLK
TAIL = SHARD % BLK // 128
LAST = SHARD % 128
PAD = 200


NST = 6


def step_kernel(sc, g0, g1, g2, g3, g4, g5, m_in, v_in, w_in, out, m_out, v_out, w_out,
                acc, r1, r2, r3, stage, raw, mine,
                dsend, drecv, own, s1, q1, s2, q2, s3, q3, lsem, isend, irecv, asend, arecv):
    grads = (g0, g1, g2, g3, g4, g5)
    me = my_id()
    delta = deltas(me)
    peers = [coords(me + x) for x in delta]
    entry_barrier(peers)
    partner = peers[0]

    def from_grads(start, go):
        for k in range(6):
            @pl.when((start >= TOFF[k]) & (start + SUB <= TOFF[k + 1]))
            def _(k=k):
                go(grads[k].at[pl.ds(pl.multiple_of((start - TOFF[k]) * 8, 32), CH)], 0, CH)
        for k in range(1, 6):
            @pl.when((start < TOFF[k]) & (start + SUB > TOFF[k]))
            def _(k=k):
                def body(j, _):
                    @pl.when(start + j * PIECE < TOFF[k])
                    def _():
                        go(grads[k - 1].at[pl.ds(pl.multiple_of((start + j * PIECE - TOFF[k - 1]) * 8, 32), PIECE * 8)],
                           j * PIECE * 8, PIECE * 8)

                    @pl.when(start + j * PIECE >= TOFF[k])
                    def _():
                        go(grads[k].at[pl.ds(pl.multiple_of((start + j * PIECE - TOFF[k]) * 8, 32), PIECE * 8)],
                           j * PIECE * 8, PIECE * 8)
                    return 0
                lax.fori_loop(0, SUB // PIECE, body, 0)

    def chunk(ref, i):
        return ref.at[pl.ds(pl.multiple_of(i * CH, CH), CH)]

    def tile_of(n, k, core):
        half = 1 - n // 8
        i = n % 8
        j = i // 2
        d1, d2, d3 = COLORS[k]
        w = me + core * delta[0] + half * delta[d1] + (1 - j // 2) * delta[d2] + (1 - j % 2) * delta[d3]
        return win_start(w) + (2 * k + i % 2) * SUB

    def d2d_start(n):
        for k in range(3):
            c = n * 3 + k

            def go(src, off, rows, c=c):
                pltpu.make_async_remote_copy(
                    src, acc.at[pl.ds(pl.multiple_of(c * CH + off, 32), rows)], dsend.at[c], drecv.at[c],
                    device_id=partner, device_id_type=MESH).start()
            from_grads(tile_of(n, k, 1), go)

    def own_start(n):
        for k in range(3):
            slot = (n % 2) * 3 + k

            def go(src, off, rows, slot=slot):
                pltpu.make_async_copy(src, stage.at[pl.ds(pl.multiple_of(slot * CH + off, 32), rows)], own.at[slot]).start()
            from_grads(tile_of(n, k, 0), go)

    def add(dst, i, srcs):
        def body(t, _):
            o = t * 32
            x = dst[pl.ds(pl.multiple_of(i * CH + o, 32), 32), :]
            for ref, s in srcs:
                x = x + ref[pl.ds(pl.multiple_of(s * CH + o, 32), 32), :]
            dst[pl.ds(pl.multiple_of(i * CH + o, 32), 32), :] = x
            return 0
        lax.fori_loop(0, CH // 32, body, 0)

    def hop(src, i, dst, j, ssem, rsem, k, step):
        return pltpu.make_async_remote_copy(
            chunk(src, i), chunk(dst, j), ssem.at[j], rsem.at[j],
            device_id=peers[COLORS[k][step]], device_id_type=MESH)

    def d2d_desc(c):
        return pltpu.make_async_remote_copy(chunk(acc, c), chunk(acc, c), dsend.at[c], drecv.at[c],
                                            device_id=partner, device_id_type=MESH)

    AHEAD = 4
    own_start(0)
    for n in range(AHEAD):
        d2d_start(n)
        if n == 0:
            own_start(1)

    def first(n, _):
        @pl.when(n + AHEAD < 16)
        def _():
            d2d_start(n + AHEAD)
        for k in range(3):
            c = n * 3 + k
            slot = (n % 2) * 3 + k
            pltpu.make_async_copy(chunk(stage, slot), chunk(stage, slot), own.at[slot]).wait()
            d2d_desc(c).wait_recv()
            add(acc, c, ((stage, slot),))

            @pl.when(n < 8)
            def _():
                hop(acc, c, r1, c, s1, q1, k, 0).start()

        @pl.when(n + 2 < 16)
        def _():
            own_start(n + 2)
        return 0
    lax.fori_loop(0, 16, first, 0)

    def second(i, _):
        for k in range(3):
            c = i * 3 + k
            hop(acc, c, r1, c, s1, q1, k, 0).wait_recv()
            add(acc, 24 + c, ((r1, c),))
            hop(acc, 24 + c, r2, c, s2, q2, k, 1).start()
        return 0
    lax.fori_loop(0, 4, second, 0)

    start = me * SHARD
    off = start % 128
    base = win_start(me)
    q = (start - off) // 128 - 8 * base
    flat_rows = acc
    lane8 = lax.broadcasted_iota(jnp.int32, (8, 128), 1)

    def each_block(one):
        for k in range(6):
            n = PER[k]
            e0 = start - TOFF[k] * 1024
            lo = jnp.minimum(jnp.maximum(e0, 0) // (n * 1024), NBLK[k])
            hi = jnp.minimum((jnp.maximum(e0 + SHARD, 0) + n * 1024 - 1) // (n * 1024), NBLK[k])
            t0 = TOFF[k] - base

            def body(b, _, t0=t0, n=n):
                row = pl.multiple_of((t0 + b * n) * 8, 8)
                if n == 22:
                    @pl.when(row + 8 * n <= WR)
                    def _():
                        one(row, n, n)

                    @pl.when(row + 8 * n > WR)
                    def _():
                        one(row, n, 8)
                else:
                    one(row, n, n)
                return 0
            lax.fori_loop(lo, hi, body, 0)

    def pieces(one):
        def body(i, _):
            one(pl.multiple_of(i * (BLK // 128), 8), BLK // 128, 128, pl.multiple_of(i * BLK, BLK))
            return 0
        lax.fori_loop(0, NB, body, 0)
        one(NB * BLK // 128, TAIL, 128, NB * BLK)
        one(NB * BLK // 128 + TAIL, 1, LAST, NB * BLK + TAIL * 128)

    def to_tile_order(src, dst, first):
        load = pltpu.make_async_copy(src, raw, lsem.at[0])
        load.start()
        load.wait()

        def shift(row, rows, cols, e):
            x = raw[pl.ds(e, rows * cols)].reshape(rows, cols)
            if cols < 128:
                x = jnp.concatenate([x, jnp.zeros((rows, 128 - cols), F32)], axis=1)
            flat_rows[pl.ds(row + PAD, rows), :] = pltpu.roll(x, off, 1)
        pieces(shift)

        def block(row, n, todo):
            for j in range(todo):
                x = flat_rows[pl.ds(row + j - q + PAD, 8, stride=n), :]
                y = flat_rows[pl.ds(row + j - q + PAD - 1, 8, stride=n), :]
                dst[pl.ds(pl.multiple_of(first + row + 8 * j, 8), 8), :] = jnp.where(lane8 >= off, x, y)
        each_block(block)

    def to_flat_order(src, first, dst):
        def block(row, n, todo):
            for j in range(todo):
                flat_rows[pl.ds(row + j, 8, stride=n), :] = src[pl.ds(pl.multiple_of(first + row + 8 * j, 8), 8), :]
        each_block(block)
        back = (128 - off) % 128

        def shift(row, rows, cols, e):
            lane = lax.broadcasted_iota(jnp.int32, (rows, 128), 1)
            x = pltpu.roll(flat_rows[pl.ds(q + row, rows), :], back, 1)
            y = pltpu.roll(flat_rows[pl.ds(q + row + 1, rows), :], back, 1)
            raw[pl.ds(e, rows * cols)] = jnp.where(lane < 128 - off, x, y)[:, :cols].reshape(rows * cols)
        pieces(shift)
        store = pltpu.make_async_copy(raw, dst, lsem.at[0])
        store.start()
        store.wait()

    def free1(i, _):
        for k in range(3):
            hop(acc, i * 3 + k, r1, i * 3 + k, s1, q1, k, 0).wait_send()
        return 0
    lax.fori_loop(0, 4, free1, 0)
    state = ((m_in, m_out, r1, 0), (v_in, v_out, r1, WR), (w_in, w_out, stage, 0))
    for src, _, dst, first in state:
        to_tile_order(src, dst, first)

    def third(i, _):
        for k in range(3):
            c = i * 3 + k
            hop(acc, 12 + c, r1, 12 + c, s1, q1, k, 0).wait_recv()
            hop(acc, c, r2, c, s2, q2, k, 1).wait_recv()
            add(acc, 36 + c, ((r1, 12 + c), (r2, c)))
            hop(acc, 36 + c, r3, c, s3, q3, k, 2).start()
        return 0
    lax.fori_loop(0, 2, third, 0)

    def fourth(i, _):
        for k in range(3):
            c = i * 3 + k
            hop(acc, 18 + c, r1, 18 + c, s1, q1, k, 0).wait_recv()
            hop(acc, 6 + c, r2, 6 + c, s2, q2, k, 1).wait_recv()
            add(acc, 42 + c, ((r1, 18 + c), (r2, 6 + c)))
        return 0
    lax.fori_loop(0, 2, fourth, 0)

    def slot(k, s, e):
        d1, d2, d3 = COLORS[k]
        w = me + (e % 2) * delta[d1] + (e // 2 % 2) * delta[d2] + (e // 4) * delta[d3]
        return out.at[pl.ds(pl.multiple_of(w * WR + (2 * k + s) * CH, 32), CH)]

    def mine_at(k, s):
        return mine.at[pl.ds((2 * k + s) * CH, CH)]

    def send(src, dst, k, s, e, step):
        i = (k * 2 + s) * 8 + e + (1 << step)
        return pltpu.make_async_remote_copy(src, dst, isend.at[i], irecv.at[i],
                                            device_id=peers[COLORS[k][step]], device_id_type=MESH)

    def across(src, dst, k, s, e):
        i = (k * 2 + s) * 8 + e
        return pltpu.make_async_remote_copy(src, dst, asend.at[i], arecv.at[i], device_id=peers[0], device_id_type=MESH)

    lr, b1, b2, eps, ic1, ic2 = (sc[i] for i in range(6))

    def fifth(i, _):
        for k in range(3):
            c = i * 3 + k
            hop(acc, 36 + c, r3, c, s3, q3, k, 2).wait_recv()

            def adam(t, _, c=c, k=k):
                o = t * 32
                g = (acc[pl.ds(pl.multiple_of((42 + c) * CH + o, 32), 32), :]
                     + r3[pl.ds(pl.multiple_of(c * CH + o, 32), 32), :]) * (1.0 / NDEV)
                p = (2 * k + i) * CH + o
                here = pl.ds(pl.multiple_of(p, 32), 32)
                there = pl.ds(pl.multiple_of(WR + p, 32), 32)
                m = b1 * r1[here, :] + (1.0 - b1) * g
                v = b2 * r1[there, :] + (1.0 - b2) * (g * g)
                w = stage[here, :] - lr * (m * ic1) / (jnp.sqrt(v * ic2) + eps)
                r1[here, :] = m
                r1[there, :] = v
                stage[here, :] = w
                mine[here, :] = w.astype(BF16)
                return 0
            lax.fori_loop(0, CH // 32, adam, 0)
            here = slot(k, i, 0)
            for step in range(3):
                send(mine_at(k, i), here, k, i, 0, step).start()
            across(mine_at(k, i), here, k, i, 0).start()
        return 0
    lax.fori_loop(0, 2, fifth, 0)
    keep = pltpu.make_async_copy(mine, out.at[pl.ds(pl.multiple_of(me * WR, 32), WR)], lsem.at[1])
    keep.start()

    ks = [(k, s) for s in range(2) for k in range(3)]

    def arrive(e, _):
        for k, s in ks:
            here = slot(k, s, e)
            send(here, here, k, s, e - 1, 0).wait_recv()
            for step in (1, 2):
                @pl.when(e < (1 << step))
                def _(k=k, s=s, here=here, step=step):
                    send(here, here, k, s, e, step).start()
            across(here, here, k, s, e).start()
        return 0

    for (_, dst, src, first), (lo, hi) in zip(state, ((1, 2), (2, 4), (4, 8))):
        to_flat_order(src, first, dst)
        lax.fori_loop(lo, hi, arrive, 0)

    def finish(i, _):
        any_chunk = mine_at(0, 0)

        def desc(ss, rs):
            return pltpu.make_async_remote_copy(any_chunk, any_chunk, ss.at[i], rs.at[i],
                                                device_id=peers[0], device_id_type=MESH)
        desc(asend, arecv).wait_recv()
        desc(asend, arecv).wait_send()

        @pl.when(i % 8 > 0)
        def _():
            desc(isend, irecv).wait_send()
        return 0
    lax.fori_loop(0, 48, finish, 0)
    keep.wait()

    def drain(i, _):
        for k in range(3):
            c = i * 3 + k

            @pl.when(i < 2)
            def _(k=k, c=c):
                hop(acc, c, r3, c, s3, q3, k, 2).wait_send()
            hop(acc, c, r2, c, s2, q2, k, 1).wait_send()
            hop(acc, 12 + c, r1, 12 + c, s1, q1, k, 0).wait_send()
        return 0
    lax.fori_loop(0, 4, drain, 0)

    def draind(c, _):
        d2d_desc(c).wait_send()
        return 0
    lax.fori_loop(0, 48, draind, 0)


ANY = pl.BlockSpec(memory_space=pl.ANY)


def step_call(scal, grads, m, v, w):
    dma = pltpu.SemaphoreType.DMA
    flat = jax.ShapeDtypeStruct((SHARD,), F32)
    return pl.pallas_call(
        step_kernel,
        out_shape=(jax.ShapeDtypeStruct((NDEV * WR, 128), BF16), flat, flat, flat),
        in_specs=[pl.BlockSpec(memory_space=pltpu.SMEM)] + [ANY] * 9,
        out_specs=[ANY] * 4,
        scratch_shapes=[
            pltpu.VMEM((48 * CH, 128), F32), pltpu.VMEM((24 * CH, 128), F32), pltpu.VMEM((12 * CH, 128), F32),
            pltpu.VMEM((6 * CH, 128), F32), pltpu.VMEM((NST * CH, 128), F32),
            pltpu.VMEM((SHARD,), F32), pltpu.VMEM((WR, 128), BF16),
            dma((48,)), dma((48,)), dma((NST,)), dma((24,)), dma((24,)), dma((12,)), dma((12,)), dma((6,)), dma((6,)),
            dma((2,)), dma((48,)), dma((48,)), dma((48,)), dma((48,)),
        ],
        compiler_params=pltpu.CompilerParams(collective_id=0, has_side_effects=True, vmem_limit_bytes=67043328),
        name="step",
    )(scal, *grads, m, v, w)


BSTART = [block_start(w) for w in range(NDEV)]


def put_kernel(slots, m, v, w, m_out, v_out, w_out, o0, o1, o2, o3, o4, o5, buf, mb, vb, wb, isem, osem):
    outs = (o0, o1, o2, o3, o4, o5)
    state = ((m, mb, m_out), (v, vb, v_out), (w, wb, w_out))
    loads = [pltpu.make_async_copy(slots.at[pl.ds(w * WR, WR)], buf.at[pl.ds(w * WR, WR)], isem.at[w])
             for w in range(NDEV)]
    loads += [pltpu.make_async_copy(a, b, isem.at[NDEV + i]) for i, (a, b, _) in enumerate(state)]
    for c in loads:
        c.start()
    stores = []
    for w in range(NDEV):
        loads[w].wait()
        t, n, _ = BSTART[w]
        bound = w * SHARD - t * 1024
        if bound > 0:
            a, b = win_start(w), win_start(w - 1)
            p = (lax.broadcasted_iota(jnp.int32, (8, 128), 0) * (n * 128)
                 + lax.broadcasted_iota(jnp.int32, (8, 128), 1))
            for j in range(n):
                if j * 128 < bound:
                    here = pl.ds(w * WR + (t + j - a) * 8, 8)
                    x = buf[here, :].astype(F32)
                    y = buf[pl.ds((w - 1) * WR + (t + j - b) * 8, 8), :].astype(F32)
                    buf[here, :] = jnp.where(p + j * 128 < bound, y, x).astype(BF16)
        end = BSTART[w + 1][0] if w + 1 < NDEV else TOFF[6]
        for k in range(6):
            lo, hi = max(t, TOFF[k]), min(end, TOFF[k + 1])
            if lo < hi:
                c = pltpu.make_async_copy(
                    buf.at[pl.ds(w * WR + (lo - win_start(w)) * 8, (hi - lo) * 8)],
                    outs[k].at[pl.ds((lo - TOFF[k]) * 8, (hi - lo) * 8)], osem.at[len(stores)])
                c.start()
                stores.append(c)
    for i, (_, b, o) in enumerate(state):
        loads[NDEV + i].wait()
        c = pltpu.make_async_copy(b, o, osem.at[len(stores)])
        c.start()
        stores.append(c)
    for c in stores:
        c.wait()


def put(slots, m, v, w):
    flat = jax.ShapeDtypeStruct((SHARD,), F32)
    return pl.pallas_call(
        put_kernel,
        out_shape=(flat,) * 3 + tuple(jax.ShapeDtypeStruct(((TOFF[k + 1] - TOFF[k]) * 8, 128), BF16) for k in range(6)),
        in_specs=[ANY] * 4,
        out_specs=[ANY] * 9,
        scratch_shapes=[pltpu.VMEM((NDEV * WR, 128), BF16)] + [pltpu.VMEM((SHARD,), F32)] * 3 + [
                        pltpu.SemaphoreType.DMA((NDEV + 3,)),
                        pltpu.SemaphoreType.DMA((32,))],
        compiler_params=pltpu.CompilerParams(vmem_limit_bytes=67043328),
        name="put",
    )(slots, m, v, w)


def to_tiles(x):
    r, c = x.shape
    return x.reshape(r // 8, 8, c // 128, 128).transpose(0, 2, 1, 3).reshape(r * c // 128, 128)


def from_tiles(x, r, c):
    return x.reshape(r // 8, c // 128, 8, 128).transpose(0, 2, 1, 3).reshape(r, c)


def solution(mesh):
    def body(g_emb, g_qkv, g_o, g_w1, g_w2, g_bqkv, g_b1, g_dvec, m, v, w, lr, beta1, beta2, eps, step):
        big = [to_tiles(x.reshape(rc)) for x, rc in zip((g_emb, g_qkv, g_o, g_w1, g_w2), BIG)]
        small = jnp.concatenate([g_bqkv.reshape(-1, 128), g_b1.reshape(-1, 128), g_dvec.reshape(-1, 128),
                                 jnp.zeros((SMALL_TILES * 8 - sum(SMALL) // 128, 128), F32)])
        t = step.astype(F32)
        scal = jnp.stack([lr, beta1, beta2, eps, 1.0 / (1.0 - beta1 ** t), 1.0 / (1.0 - beta2 ** t)])
        m_new, v_new, w_new, *outs = put(*step_call(scal, (*big, small), m, v, w))
        wbs = [from_tiles(o, *rc) for o, rc in zip(outs, BIG)]
        r = [0, SMALL[0] // 128, (SMALL[0] + SMALL[1]) // 128, sum(SMALL) // 128]
        s = outs[5]
        return (m_new, v_new, w_new, wbs[0], wbs[1][None], wbs[2][None], wbs[3][None], wbs[4][None],
                s[r[0]:r[1]].reshape(1, -1), s[r[1]:r[2]].reshape(1, -1), s[r[2]:r[3]].reshape(1, 6, 1024))

    g3 = P(AXES, None, None)
    g4 = P(AXES, None, None, None)
    flat = P(AXES)
    rep = P()
    in_specs = (g3, g4, g4, g4, g4, g3, g3, g4, flat, flat, flat, rep, rep, rep, rep, rep)
    out_specs = (flat, flat, flat, rep, rep, rep, rep, rep, rep, rep, rep)
    return jax.shard_map(body, mesh=mesh, in_specs=in_specs, out_specs=out_specs, check_vma=False)
```

```python
import functools
import math
import jax
import jax.numpy as jnp
from jax import lax
from jax.experimental import pallas as pl
from jax.experimental.pallas import tpu as pltpu
from jax.sharding import PartitionSpec as P

AXES = ("outer", "inner")
MESH = pl.DeviceIdType.MESH
F32, BF16 = jnp.float32, jnp.bfloat16
NDEV = 16
SHARD = 885488
BIG = ((4096, 1024), (1024, 3072), (1024, 1024), (1024, 2816), (2816, 1024))
PER = tuple(c // 128 for _, c in BIG) + (1,)
SMALL = (3072, 2816, 6144)
SMALL_TILES = 32
TOFF = [0]
for _r, _c in BIG:
    TOFF.append(TOFF[-1] + _r * _c // 1024)
TOFF.append(TOFF[-1] + SMALL_TILES)
NBLK = tuple((TOFF[k + 1] - TOFF[k]) // PER[k] for k in range(6))

WIN = 888
SUB = 148
CH = SUB * 8
WR = WIN * 8
PIECE = 4
COLORS = ((1, 2, 3), (2, 3, 1), (3, 1, 2))


def win_start(w):
    def ge(t):
        return (w + 16 - t) // 16
    return 864 * w + 8 * (ge(9) - ge(5) - ge(10) + 2 * ge(11) - ge(12) + ge(13))


def block_start(w):
    e = w * SHARD
    t = e // 1024
    k = max(i for i in range(6) if TOFF[i] <= t)
    n = PER[k]
    return TOFF[k] + ((e - TOFF[k] * 1024) // (n * 1024)) * n, n, k


def my_id():
    return lax.axis_index("outer") * 8 + lax.axis_index("inner")


def coords(d):
    return (d // 8, d % 8)


def deltas(me):
    return [(1 - 2 * ((me // (1 << d)) % 2)) * (1 << d) for d in range(4)]


def entry_barrier(peers):
    sem = pltpu.get_barrier_semaphore()
    for p in peers:
        pl.semaphore_signal(sem, inc=1, device_id=p, device_id_type=MESH)
    pl.semaphore_wait(sem, 4)


BLK = 4096
NB = SHARD // BLK
TAIL = SHARD % BLK // 128
LAST = SHARD % 128
PAD = 200
LROWS = 7424


NST = 6


def each_block(me, one):
    start = me * SHARD
    base = win_start(me)
    for k in range(6):
        n = PER[k]
        e0 = start - TOFF[k] * 1024
        lo = jnp.minimum(jnp.maximum(e0, 0) // (n * 1024), NBLK[k])
        hi = jnp.minimum((jnp.maximum(e0 + SHARD, 0) + n * 1024 - 1) // (n * 1024), NBLK[k])
        t0 = TOFF[k] - base

        def body(b, _, t0=t0, n=n):
            row = pl.multiple_of((t0 + b * n) * 8, 8)
            if n == 22:
                @pl.when(row + 8 * n <= WR)
                def _():
                    one(row, n, n)

                @pl.when(row + 8 * n > WR)
                def _():
                    one(row, n, 8)
            else:
                one(row, n, n)
            return 0
        lax.fori_loop(lo, hi, body, 0)


def pieces(one):
    def body(i, _):
        one(pl.multiple_of(i * (BLK // 128), 8), BLK // 128, 128, pl.multiple_of(i * BLK, BLK))
        return 0
    lax.fori_loop(0, NB, body, 0)
    one(NB * BLK // 128, TAIL, 128, NB * BLK)
    one(NB * BLK // 128 + TAIL, 1, LAST, NB * BLK + TAIL * 128)


def rs_kernel(sc, g0, g1, g2, g3, g4, g5, m_in, v_in, w_in, wb_out, m_out, v_out, w_out,
                acc, r1, r2, r3, stage, raw, mine,
                dsend, drecv, own, s1, q1, s2, q2, s3, q3, lsem, osem):
    grads = (g0, g1, g2, g3, g4, g5)
    me = my_id()
    delta = deltas(me)
    peers = [coords(me + x) for x in delta]
    entry_barrier(peers)
    partner = peers[0]

    def from_grads(start, go):
        for k in range(6):
            @pl.when((start >= TOFF[k]) & (start + SUB <= TOFF[k + 1]))
            def _(k=k):
                go(grads[k].at[pl.ds(pl.multiple_of((start - TOFF[k]) * 8, 32), CH)], 0, CH)
        for k in range(1, 6):
            @pl.when((start < TOFF[k]) & (start + SUB > TOFF[k]))
            def _(k=k):
                def body(j, _):
                    @pl.when(start + j * PIECE < TOFF[k])
                    def _():
                        go(grads[k - 1].at[pl.ds(pl.multiple_of((start + j * PIECE - TOFF[k - 1]) * 8, 32), PIECE * 8)],
                           j * PIECE * 8, PIECE * 8)

                    @pl.when(start + j * PIECE >= TOFF[k])
                    def _():
                        go(grads[k].at[pl.ds(pl.multiple_of((start + j * PIECE - TOFF[k]) * 8, 32), PIECE * 8)],
                           j * PIECE * 8, PIECE * 8)
                    return 0
                lax.fori_loop(0, SUB // PIECE, body, 0)

    def chunk(ref, i):
        return ref.at[pl.ds(pl.multiple_of(i * CH, CH), CH)]

    def tile_of(n, k, core):
        half = 1 - n // 8
        i = n % 8
        j = i // 2
        d1, d2, d3 = COLORS[k]
        w = me + core * delta[0] + half * delta[d1] + (1 - j // 2) * delta[d2] + (1 - j % 2) * delta[d3]
        return win_start(w) + (2 * k + i % 2) * SUB

    def d2d_start(n):
        for k in range(3):
            c = n * 3 + k

            def go(src, off, rows, c=c):
                pltpu.make_async_remote_copy(
                    src, acc.at[pl.ds(pl.multiple_of(c * CH + off, 32), rows)], dsend.at[c], drecv.at[c],
                    device_id=partner, device_id_type=MESH).start()
            from_grads(tile_of(n, k, 1), go)

    def own_start(n):
        for k in range(3):
            slot = (n % 2) * 3 + k

            def go(src, off, rows, slot=slot):
                pltpu.make_async_copy(src, stage.at[pl.ds(pl.multiple_of(slot * CH + off, 32), rows)], own.at[slot]).start()
            from_grads(tile_of(n, k, 0), go)

    def add(dst, i, srcs):
        def body(t, _):
            o = t * 32
            x = dst[pl.ds(pl.multiple_of(i * CH + o, 32), 32), :]
            for ref, s in srcs:
                x = x + ref[pl.ds(pl.multiple_of(s * CH + o, 32), 32), :]
            dst[pl.ds(pl.multiple_of(i * CH + o, 32), 32), :] = x
            return 0
        lax.fori_loop(0, CH // 32, body, 0)

    def hop(src, i, dst, j, ssem, rsem, k, step):
        return pltpu.make_async_remote_copy(
            chunk(src, i), chunk(dst, j), ssem.at[j], rsem.at[j],
            device_id=peers[COLORS[k][step]], device_id_type=MESH)

    def d2d_desc(c):
        return pltpu.make_async_remote_copy(chunk(acc, c), chunk(acc, c), dsend.at[c], drecv.at[c],
                                            device_id=partner, device_id_type=MESH)

    AHEAD = 4
    own_start(0)
    for n in range(AHEAD):
        d2d_start(n)
        if n == 0:
            own_start(1)

    def first(n, _):
        @pl.when(n + AHEAD < 16)
        def _():
            d2d_start(n + AHEAD)
        for k in range(3):
            c = n * 3 + k
            slot = (n % 2) * 3 + k
            pltpu.make_async_copy(chunk(stage, slot), chunk(stage, slot), own.at[slot]).wait()
            d2d_desc(c).wait_recv()
            add(acc, c, ((stage, slot),))

            @pl.when(n < 8)
            def _():
                hop(acc, c, r1, c, s1, q1, k, 0).start()

        @pl.when(n + 2 < 16)
        def _():
            own_start(n + 2)
        return 0
    lax.fori_loop(0, 16, first, 0)

    def second(i, _):
        for k in range(3):
            c = i * 3 + k
            hop(acc, c, r1, c, s1, q1, k, 0).wait_recv()
            add(acc, 24 + c, ((r1, c),))
            hop(acc, 24 + c, r2, c, s2, q2, k, 1).start()
        return 0
    lax.fori_loop(0, 4, second, 0)

    start = me * SHARD
    off = start % 128
    base = win_start(me)
    q = (start - off) // 128 - 8 * base
    flat_rows = acc
    lane8 = lax.broadcasted_iota(jnp.int32, (8, 128), 1)

    def to_tile_order(src, dst, first):
        load = pltpu.make_async_copy(src, raw, lsem.at[0])
        load.start()
        load.wait()

        def shift(row, rows, cols, e):
            x = raw[pl.ds(e, rows * cols)].reshape(rows, cols)
            if cols < 128:
                x = jnp.concatenate([x, jnp.zeros((rows, 128 - cols), F32)], axis=1)
            flat_rows[pl.ds(row + PAD, rows), :] = pltpu.roll(x, off, 1)
        pieces(shift)

        def block(row, n, todo):
            for j in range(todo):
                x = flat_rows[pl.ds(row + j - q + PAD, 8, stride=n), :]
                y = flat_rows[pl.ds(row + j - q + PAD - 1, 8, stride=n), :]
                dst[pl.ds(pl.multiple_of(first + row + 8 * j, 8), 8), :] = jnp.where(lane8 >= off, x, y)
        each_block(me, block)

    def free1(i, _):
        for k in range(3):
            hop(acc, i * 3 + k, r1, i * 3 + k, s1, q1, k, 0).wait_send()
        return 0
    lax.fori_loop(0, 4, free1, 0)
    state = ((m_in, r1, 0), (v_in, r1, WR), (w_in, stage, 0))
    for src, dst, first in state:
        to_tile_order(src, dst, first)

    def third(i, _):
        for k in range(3):
            c = i * 3 + k
            hop(acc, 12 + c, r1, 12 + c, s1, q1, k, 0).wait_recv()
            hop(acc, c, r2, c, s2, q2, k, 1).wait_recv()
            add(acc, 36 + c, ((r1, 12 + c), (r2, c)))
            hop(acc, 36 + c, r3, c, s3, q3, k, 2).start()
        return 0
    lax.fori_loop(0, 2, third, 0)

    def fourth(i, _):
        for k in range(3):
            c = i * 3 + k
            hop(acc, 18 + c, r1, 18 + c, s1, q1, k, 0).wait_recv()
            hop(acc, 6 + c, r2, 6 + c, s2, q2, k, 1).wait_recv()
            add(acc, 42 + c, ((r1, 18 + c), (r2, 6 + c)))
        return 0
    lax.fori_loop(0, 2, fourth, 0)

    def results(k, i):
        p = (2 * k + i) * CH
        return [pltpu.make_async_copy(src.at[pl.ds(pl.multiple_of(first + p, 32), CH)],
                                      dst.at[pl.ds(pl.multiple_of(p, 32), CH)], osem.at[j * 6 + 2 * k + i])
                for j, (src, first, dst) in enumerate(
                    ((mine, 0, wb_out), (r1, 0, m_out), (r1, WR, v_out), (stage, 0, w_out)))]

    lr, b1, b2, eps, ic1, ic2 = (sc[i] for i in range(6))

    def fifth(i, _):
        for k in range(3):
            c = i * 3 + k
            hop(acc, 36 + c, r3, c, s3, q3, k, 2).wait_recv()

            def adam(t, _, c=c, k=k):
                o = t * 32
                g = (acc[pl.ds(pl.multiple_of((42 + c) * CH + o, 32), 32), :]
                     + r3[pl.ds(pl.multiple_of(c * CH + o, 32), 32), :]) * (1.0 / NDEV)
                p = (2 * k + i) * CH + o
                here = pl.ds(pl.multiple_of(p, 32), 32)
                there = pl.ds(pl.multiple_of(WR + p, 32), 32)
                m = b1 * r1[here, :] + (1.0 - b1) * g
                v = b2 * r1[there, :] + (1.0 - b2) * (g * g)
                w = stage[here, :] - lr * (m * ic1) / (jnp.sqrt(v * ic2) + eps)
                r1[here, :] = m
                r1[there, :] = v
                stage[here, :] = w
                mine[here, :] = w.astype(BF16)
                return 0
            lax.fori_loop(0, CH // 32, adam, 0)
            for copy in results(k, i):
                copy.start()
        return 0
    lax.fori_loop(0, 2, fifth, 0)

    def drain(i, _):
        for k in range(3):
            c = i * 3 + k

            @pl.when(i < 2)
            def _(k=k, c=c):
                hop(acc, c, r3, c, s3, q3, k, 2).wait_send()
            hop(acc, c, r2, c, s2, q2, k, 1).wait_send()
            hop(acc, 12 + c, r1, 12 + c, s1, q1, k, 0).wait_send()
        return 0
    lax.fori_loop(0, 4, drain, 0)

    def draind(c, _):
        d2d_desc(c).wait_send()
        return 0
    lax.fori_loop(0, 48, draind, 0)

    def written(i, _):
        for k in range(3):
            for copy in results(k, i):
                copy.wait()
        return 0
    lax.fori_loop(0, 2, written, 0)


ANY = pl.BlockSpec(memory_space=pl.ANY)


HBM = pl.BlockSpec(memory_space=pltpu.HBM)
VMEM = pl.BlockSpec(memory_space=pltpu.VMEM)


def reduce_and_update(scal, grads, m, v, w):
    dma = pltpu.SemaphoreType.DMA
    win = jax.ShapeDtypeStruct((WR, 128), F32)
    return pl.pallas_call(
        rs_kernel,
        out_shape=(jax.ShapeDtypeStruct((WR, 128), BF16), win, win, win),
        in_specs=[pl.BlockSpec(memory_space=pltpu.SMEM)] + [HBM] * 9,
        out_specs=[HBM] * 4,
        scratch_shapes=[
            pltpu.VMEM((48 * CH, 128), F32), pltpu.VMEM((24 * CH, 128), F32), pltpu.VMEM((12 * CH, 128), F32),
            pltpu.VMEM((6 * CH, 128), F32), pltpu.VMEM((NST * CH, 128), F32),
            pltpu.VMEM((SHARD,), F32), pltpu.VMEM((WR, 128), BF16),
            dma((48,)), dma((48,)), dma((NST,)), dma((24,)), dma((24,)), dma((12,)), dma((12,)), dma((6,)), dma((6,)),
            dma((2,)), dma((24,)),
        ],
        compiler_params=pltpu.CompilerParams(collective_id=0, has_side_effects=True, vmem_limit_bytes=67043328),
        name="rs",
    )(scal, *grads, m, v, w)


def ag_kernel(wb, m_in, v_in, w_in, m_out, v_out, w_out, out, mt, vt, wt, flat_rows, lsem, isend, irecv, asend, arecv):
    me = my_id()
    delta = deltas(me)
    peers = [coords(me + x) for x in delta]
    load = pltpu.make_async_copy(wb, out.at[pl.ds(pl.multiple_of(me * WR, 32), WR)], lsem.at[0])
    load.start()
    state = ((m_in, mt, m_out), (v_in, vt, v_out), (w_in, wt, w_out))
    loads = [pltpu.make_async_copy(src, dst.at[pl.ds(0, WR)], lsem.at[1 + i]) for i, (src, dst, _) in enumerate(state)]
    for c in loads:
        c.start()
    entry_barrier(peers)
    load.wait()
    start = me * SHARD
    off = start % 128
    q = (start - off) // 128 - 8 * win_start(me)

    def to_flat_order(src, dst):
        def block(row, n, todo):
            for j in range(todo):
                flat_rows[pl.ds(row + j, 8, stride=n), :] = src[pl.ds(pl.multiple_of(row + 8 * j, 8), 8), :]
        each_block(me, block)
        back = (128 - off) % 128

        def shift(row, rows, cols, e):
            lane = lax.broadcasted_iota(jnp.int32, (rows, 128), 1)
            x = pltpu.roll(flat_rows[pl.ds(q + row, rows), :], back, 1)
            y = pltpu.roll(flat_rows[pl.ds(q + row + 1, rows), :], back, 1)
            dst[pl.ds(e, rows * cols)] = jnp.where(lane < 128 - off, x, y)[:, :cols].reshape(rows * cols)
        pieces(shift)

    def slot(k, s, e):
        d1, d2, d3 = COLORS[k]
        w = me + (e % 2) * delta[d1] + (e // 2 % 2) * delta[d2] + (e // 4) * delta[d3]
        return out.at[pl.ds(pl.multiple_of(w * WR + (2 * k + s) * CH, 32), CH)]

    def send(src, dst, k, s, e, step):
        i = (k * 2 + s) * 8 + e + (1 << step)
        return pltpu.make_async_remote_copy(src, dst, isend.at[i], irecv.at[i],
                                            device_id=peers[COLORS[k][step]], device_id_type=MESH)

    def across(src, dst, k, s, e):
        i = (k * 2 + s) * 8 + e
        return pltpu.make_async_remote_copy(src, dst, asend.at[i], arecv.at[i], device_id=peers[0], device_id_type=MESH)

    ks = [(k, s) for s in range(2) for k in range(3)]

    for k, s in ks:
        here = slot(k, s, 0)
        for step in range(3):
            send(here, here, k, s, 0, step).start()
        across(here, here, k, s, 0).start()

    def arrive(e, _):
        for k, s in ks:
            here = slot(k, s, e)
            send(here, here, k, s, e - 1, 0).wait_recv()
            for step in (1, 2):
                @pl.when(e < (1 << step))
                def _(k=k, s=s, here=here, step=step):
                    send(here, here, k, s, e, step).start()
            across(here, here, k, s, e).start()
        return 0

    for c, (_, src, dst), (lo, hi) in zip(loads, state, ((1, 2), (2, 4), (4, 8))):
        c.wait()
        to_flat_order(src, dst)
        lax.fori_loop(lo, hi, arrive, 0)

    def finish(i, _):
        any_chunk = out.at[pl.ds(0, CH)]

        def desc(ss, rs):
            return pltpu.make_async_remote_copy(any_chunk, any_chunk, ss.at[i], rs.at[i],
                                                device_id=peers[0], device_id_type=MESH)
        desc(asend, arecv).wait_recv()
        desc(asend, arecv).wait_send()

        @pl.when(i % 8 > 0)
        def _():
            desc(isend, irecv).wait_send()
        return 0
    lax.fori_loop(0, 48, finish, 0)


def all_gather(wb, m, v, w):
    dma = pltpu.SemaphoreType.DMA
    flat = jax.ShapeDtypeStruct((SHARD,), F32)
    return pl.pallas_call(
        ag_kernel,
        out_shape=(flat, flat, flat, jax.ShapeDtypeStruct((NDEV * WR, 128), BF16)),
        in_specs=[HBM] * 4,
        out_specs=[VMEM, VMEM, VMEM, ANY],
        scratch_shapes=[pltpu.VMEM((LROWS, 128), F32)] * 4 + [dma((4,)), dma((48,)), dma((48,)), dma((48,)), dma((48,))],
        compiler_params=pltpu.CompilerParams(collective_id=1, has_side_effects=True, vmem_limit_bytes=16 << 20),
        name="ag",
    )(*(pltpu.with_memory_space_constraint(x, pltpu.HBM) for x in (wb, m, v, w)))


BSTART = [block_start(w) for w in range(NDEV)]


def put_kernel(slots, o0, o1, o2, o3, o4, o5, tmp, osem):
    outs = (o0, o1, o2, o3, o4, o5)
    stores = []

    def store(src, dst):
        c = pltpu.make_async_copy(src, dst, osem.at[len(stores)])
        c.start()
        stores.append(c)

    def store_tiles(ref, row, lo, hi):
        for k in range(6):
            a, b = max(lo, TOFF[k]), min(hi, TOFF[k + 1])
            if a < b:
                store(ref.at[pl.ds(row + (a - lo) * 8, (b - a) * 8)], outs[k].at[pl.ds((a - TOFF[k]) * 8, (b - a) * 8)])

    for d in range(NDEV):
        t, n, _ = BSTART[d]
        lo = t + n if d else 0
        store_tiles(slots, d * WR + (lo - win_start(d)) * 8, lo, BSTART[d + 1][0] if d + 1 < NDEV else TOFF[6])
    for d in range(1, NDEV):
        t, n, _ = BSTART[d]
        bound = d * SHARD - t * 1024
        p = (lax.broadcasted_iota(jnp.int32, (8, 128), 0) * (n * 128)
             + lax.broadcasted_iota(jnp.int32, (8, 128), 1))
        for j in range(n):
            x = slots[pl.ds(d * WR + (t + j - win_start(d)) * 8, 8), :]
            if j * 128 < bound:
                y = slots[pl.ds((d - 1) * WR + (t + j - win_start(d - 1)) * 8, 8), :]
                x = jnp.where(p + j * 128 < bound, y.astype(F32), x.astype(F32)).astype(BF16)
            tmp[pl.ds(d * 192 + j * 8, 8), :] = x
        store_tiles(tmp, d * 192, t, t + n)
    for c in stores:
        c.wait()


def put(slots):
    return pl.pallas_call(
        put_kernel,
        out_shape=tuple(jax.ShapeDtypeStruct(((TOFF[k + 1] - TOFF[k]) * 8, 128), BF16) for k in range(6)),
        in_specs=[VMEM],
        out_specs=[HBM] * 6,
        scratch_shapes=[pltpu.VMEM((NDEV * 192, 128), BF16), pltpu.SemaphoreType.DMA((48,))],
        compiler_params=pltpu.CompilerParams(vmem_limit_bytes=4 << 20),
        name="put",
    )(slots)


def to_tiles(x):
    r, c = x.shape
    return x.reshape(r // 8, 8, c // 128, 128).transpose(0, 2, 1, 3).reshape(r * c // 128, 128)


def from_tiles(x, r, c):
    return x.reshape(r // 8, c // 128, 8, 128).transpose(0, 2, 1, 3).reshape(r, c)


def solution(mesh):
    def body(g_emb, g_qkv, g_o, g_w1, g_w2, g_bqkv, g_b1, g_dvec, m, v, w, lr, beta1, beta2, eps, step):
        big = [to_tiles(x.reshape(rc)) for x, rc in zip((g_emb, g_qkv, g_o, g_w1, g_w2), BIG)]
        small = jnp.concatenate([g_bqkv.reshape(-1, 128), g_b1.reshape(-1, 128), g_dvec.reshape(-1, 128),
                                 jnp.zeros((SMALL_TILES * 8 - sum(SMALL) // 128, 128), F32)])
        t = step.astype(F32)
        scal = jnp.stack([lr, beta1, beta2, eps, 1.0 / (1.0 - beta1 ** t), 1.0 / (1.0 - beta2 ** t)])
        m_new, v_new, w_new, slots = all_gather(*reduce_and_update(scal, (*big, small), m, v, w))
        outs = put(slots)
        wbs = [from_tiles(o, *rc) for o, rc in zip(outs, BIG)]
        r = [0, SMALL[0] // 128, (SMALL[0] + SMALL[1]) // 128, sum(SMALL) // 128]
        s = outs[5]
        return (m_new, v_new, w_new, wbs[0], wbs[1][None], wbs[2][None], wbs[3][None], wbs[4][None],
                s[r[0]:r[1]].reshape(1, -1), s[r[1]:r[2]].reshape(1, -1), s[r[2]:r[3]].reshape(1, 6, 1024))

    g3 = P(AXES, None, None)
    g4 = P(AXES, None, None, None)
    flat = P(AXES)
    rep = P()
    in_specs = (g3, g4, g4, g4, g4, g3, g3, g4, flat, flat, flat, rep, rep, rep, rep, rep)
    out_specs = (flat, flat, flat, rep, rep, rep, rep, rep, rep, rep, rep)
    return jax.shard_map(body, mesh=mesh, in_specs=in_specs, out_specs=out_specs, check_vma=False)
```

```python
import functools
import math
import jax
import jax.numpy as jnp
from jax import lax
from jax.experimental import pallas as pl
from jax.experimental.pallas import tpu as pltpu
from jax.sharding import PartitionSpec as P

AXES = ("outer", "inner")
MESH = pl.DeviceIdType.MESH
F32, BF16 = jnp.float32, jnp.bfloat16
NDEV = 16
SHARD = 885488
BIG = ((4096, 1024), (1024, 3072), (1024, 1024), (1024, 2816), (2816, 1024))
PER = tuple(c // 128 for _, c in BIG) + (1,)
SMALL = (3072, 2816, 6144)
SMALL_TILES = 32
TOFF = [0]
for _r, _c in BIG:
    TOFF.append(TOFF[-1] + _r * _c // 1024)
TOFF.append(TOFF[-1] + SMALL_TILES)
NBLK = tuple((TOFF[k + 1] - TOFF[k]) // PER[k] for k in range(6))

WIN = 888
SUB = 148
CH = SUB * 8
WR = WIN * 8
PIECE = 4
COLORS = ((1, 2, 3), (2, 3, 1), (3, 1, 2))


def win_start(w):
    def ge(t):
        return (w + 16 - t) // 16
    return 864 * w + 8 * (ge(9) - ge(5) - ge(10) + 2 * ge(11) - ge(12) + ge(13))


def block_start(w):
    e = w * SHARD
    t = e // 1024
    k = max(i for i in range(6) if TOFF[i] <= t)
    n = PER[k]
    return TOFF[k] + ((e - TOFF[k] * 1024) // (n * 1024)) * n, n, k


def my_id():
    return lax.axis_index("outer") * 8 + lax.axis_index("inner")


def coords(d):
    return (d // 8, d % 8)


def deltas(me):
    return [(1 - 2 * ((me // (1 << d)) % 2)) * (1 << d) for d in range(4)]


def entry_barrier(peers):
    sem = pltpu.get_barrier_semaphore()
    for p in peers:
        pl.semaphore_signal(sem, inc=1, device_id=p, device_id_type=MESH)
    pl.semaphore_wait(sem, 4)


BLK = 4096
NB = SHARD // BLK
TAIL = SHARD % BLK // 128
LAST = SHARD % 128
PAD = 200
FSTEP = 32
FROWS = 6944
LROWS = 7424


NST = 6


def each_block(me, one):
    start = me * SHARD
    base = win_start(me)
    for k in range(6):
        n = PER[k]
        e0 = start - TOFF[k] * 1024
        lo = jnp.minimum(jnp.maximum(e0, 0) // (n * 1024), NBLK[k])
        hi = jnp.minimum((jnp.maximum(e0 + SHARD, 0) + n * 1024 - 1) // (n * 1024), NBLK[k])
        t0 = TOFF[k] - base

        def body(b, _, t0=t0, n=n):
            row = pl.multiple_of((t0 + b * n) * 8, 8)
            if n == 22:
                @pl.when(row + 8 * n <= WR)
                def _():
                    one(row, n, n)

                @pl.when(row + 8 * n > WR)
                def _():
                    one(row, n, 8)
            else:
                one(row, n, n)
            return 0
        lax.fori_loop(lo, hi, body, 0)


def pieces(one):
    def body(i, _):
        one(pl.multiple_of(i * (BLK // 128), 8), BLK // 128, 128, pl.multiple_of(i * BLK, BLK))
        return 0
    lax.fori_loop(0, NB, body, 0)
    one(NB * BLK // 128, TAIL, 128, NB * BLK)
    one(NB * BLK // 128 + TAIL, 1, LAST, NB * BLK + TAIL * 128)


def rs_kernel(sc, g0, g1, g2, g3, g4, g5, m_in, v_in, w_in, wb_out, m_out, v_out, w_out,
                acc, r1, r2, r3, stage, raw, mine,
                dsend, drecv, own, s1, q1, s2, q2, s3, q3, lsem, osem):
    grads = (g0, g1, g2, g3, g4, g5)
    me = my_id()
    delta = deltas(me)
    peers = [coords(me + x) for x in delta]
    entry_barrier(peers)
    partner = peers[0]

    def from_grads(start, go):
        for k in range(6):
            @pl.when((start >= TOFF[k]) & (start + SUB <= TOFF[k + 1]))
            def _(k=k):
                go(grads[k].at[pl.ds(pl.multiple_of((start - TOFF[k]) * 8, 32), CH)], 0, CH)
        for k in range(1, 6):
            @pl.when((start < TOFF[k]) & (start + SUB > TOFF[k]))
            def _(k=k):
                def body(j, _):
                    @pl.when(start + j * PIECE < TOFF[k])
                    def _():
                        go(grads[k - 1].at[pl.ds(pl.multiple_of((start + j * PIECE - TOFF[k - 1]) * 8, 32), PIECE * 8)],
                           j * PIECE * 8, PIECE * 8)

                    @pl.when(start + j * PIECE >= TOFF[k])
                    def _():
                        go(grads[k].at[pl.ds(pl.multiple_of((start + j * PIECE - TOFF[k]) * 8, 32), PIECE * 8)],
                           j * PIECE * 8, PIECE * 8)
                    return 0
                lax.fori_loop(0, SUB // PIECE, body, 0)

    def chunk(ref, i):
        return ref.at[pl.ds(pl.multiple_of(i * CH, CH), CH)]

    def tile_of(n, k, core):
        half = 1 - n // 8
        i = n % 8
        j = i // 2
        d1, d2, d3 = COLORS[k]
        w = me + core * delta[0] + half * delta[d1] + (1 - j // 2) * delta[d2] + (1 - j % 2) * delta[d3]
        return win_start(w) + (2 * k + i % 2) * SUB

    def d2d_start(n):
        for k in range(3):
            c = n * 3 + k

            def go(src, off, rows, c=c):
                pltpu.make_async_remote_copy(
                    src, acc.at[pl.ds(pl.multiple_of(c * CH + off, 32), rows)], dsend.at[c], drecv.at[c],
                    device_id=partner, device_id_type=MESH).start()
            from_grads(tile_of(n, k, 1), go)

    def own_start(n):
        for k in range(3):
            slot = (n % 2) * 3 + k

            def go(src, off, rows, slot=slot):
                pltpu.make_async_copy(src, stage.at[pl.ds(pl.multiple_of(slot * CH + off, 32), rows)], own.at[slot]).start()
            from_grads(tile_of(n, k, 0), go)

    def add(dst, i, srcs):
        def body(t, _):
            o = t * 32
            x = dst[pl.ds(pl.multiple_of(i * CH + o, 32), 32), :]
            for ref, s in srcs:
                x = x + ref[pl.ds(pl.multiple_of(s * CH + o, 32), 32), :]
            dst[pl.ds(pl.multiple_of(i * CH + o, 32), 32), :] = x
            return 0
        lax.fori_loop(0, CH // 32, body, 0)

    def hop(src, i, dst, j, ssem, rsem, k, step):
        return pltpu.make_async_remote_copy(
            chunk(src, i), chunk(dst, j), ssem.at[j], rsem.at[j],
            device_id=peers[COLORS[k][step]], device_id_type=MESH)

    def d2d_desc(c):
        return pltpu.make_async_remote_copy(chunk(acc, c), chunk(acc, c), dsend.at[c], drecv.at[c],
                                            device_id=partner, device_id_type=MESH)

    AHEAD = 4
    own_start(0)
    for n in range(AHEAD):
        d2d_start(n)
        if n == 0:
            own_start(1)

    def first(n, _):
        @pl.when(n + AHEAD < 16)
        def _():
            d2d_start(n + AHEAD)
        for k in range(3):
            c = n * 3 + k
            slot = (n % 2) * 3 + k
            pltpu.make_async_copy(chunk(stage, slot), chunk(stage, slot), own.at[slot]).wait()
            d2d_desc(c).wait_recv()
            add(acc, c, ((stage, slot),))

            @pl.when(n < 8)
            def _():
                hop(acc, c, r1, c, s1, q1, k, 0).start()

        @pl.when(n + 2 < 16)
        def _():
            own_start(n + 2)
        return 0
    lax.fori_loop(0, 16, first, 0)

    def second(i, _):
        for k in range(3):
            c = i * 3 + k
            hop(acc, c, r1, c, s1, q1, k, 0).wait_recv()
            add(acc, 24 + c, ((r1, c),))
            hop(acc, 24 + c, r2, c, s2, q2, k, 1).start()
        return 0
    lax.fori_loop(0, 4, second, 0)

    start = me * SHARD
    off = start % 128
    base = win_start(me)
    q = (start - off) // 128 - 8 * base
    flat_rows = acc
    lane8 = lax.broadcasted_iota(jnp.int32, (8, 128), 1)

    def to_tile_order(src, dst, first):
        load = pltpu.make_async_copy(src, raw, lsem.at[0])
        load.start()
        load.wait()

        def shift(row, rows, cols, e):
            x = raw[pl.ds(e, rows * cols)].reshape(rows, cols)
            if cols < 128:
                x = jnp.concatenate([x, jnp.zeros((rows, 128 - cols), F32)], axis=1)
            flat_rows[pl.ds(row + PAD, rows), :] = pltpu.roll(x, off, 1)
        pieces(shift)

        def block(row, n, todo):
            for j in range(todo):
                x = flat_rows[pl.ds(row + j - q + PAD, 8, stride=n), :]
                y = flat_rows[pl.ds(row + j - q + PAD - 1, 8, stride=n), :]
                dst[pl.ds(pl.multiple_of(first + row + 8 * j, 8), 8), :] = jnp.where(lane8 >= off, x, y)
        each_block(me, block)

    def free1(i, _):
        for k in range(3):
            hop(acc, i * 3 + k, r1, i * 3 + k, s1, q1, k, 0).wait_send()
        return 0
    lax.fori_loop(0, 4, free1, 0)
    state = ((m_in, r1, 0), (v_in, r1, WR), (w_in, stage, 0))
    for src, dst, first in state:
        to_tile_order(src, dst, first)

    def third(i, _):
        for k in range(3):
            c = i * 3 + k
            hop(acc, 12 + c, r1, 12 + c, s1, q1, k, 0).wait_recv()
            hop(acc, c, r2, c, s2, q2, k, 1).wait_recv()
            add(acc, 36 + c, ((r1, 12 + c), (r2, c)))
            hop(acc, 36 + c, r3, c, s3, q3, k, 2).start()
        return 0
    lax.fori_loop(0, 2, third, 0)

    def fourth(i, _):
        for k in range(3):
            c = i * 3 + k
            hop(acc, 18 + c, r1, 18 + c, s1, q1, k, 0).wait_recv()
            hop(acc, 6 + c, r2, 6 + c, s2, q2, k, 1).wait_recv()
            add(acc, 42 + c, ((r1, 18 + c), (r2, 6 + c)))
        return 0
    lax.fori_loop(0, 2, fourth, 0)

    def results(k, i):
        p = (2 * k + i) * CH
        return [pltpu.make_async_copy(src.at[pl.ds(pl.multiple_of(first + p, 32), CH)],
                                      dst.at[pl.ds(pl.multiple_of(p, 32), CH)], osem.at[j * 6 + 2 * k + i])
                for j, (src, first, dst) in enumerate(
                    ((mine, 0, wb_out), (r1, 0, m_out), (r1, WR, v_out), (stage, 0, w_out)))]

    lr, b1, b2, eps, ic1, ic2 = (sc[i] for i in range(6))

    def fifth(i, _):
        for k in range(3):
            c = i * 3 + k
            hop(acc, 36 + c, r3, c, s3, q3, k, 2).wait_recv()

            def adam(t, _, c=c, k=k):
                o = t * 32
                g = (acc[pl.ds(pl.multiple_of((42 + c) * CH + o, 32), 32), :]
                     + r3[pl.ds(pl.multiple_of(c * CH + o, 32), 32), :]) * (1.0 / NDEV)
                p = (2 * k + i) * CH + o
                here = pl.ds(pl.multiple_of(p, 32), 32)
                there = pl.ds(pl.multiple_of(WR + p, 32), 32)
                m = b1 * r1[here, :] + (1.0 - b1) * g
                v = b2 * r1[there, :] + (1.0 - b2) * (g * g)
                w = stage[here, :] - lr * (m * ic1) / (jnp.sqrt(v * ic2) + eps)
                r1[here, :] = m
                r1[there, :] = v
                stage[here, :] = w
                mine[here, :] = w.astype(BF16)
                return 0
            lax.fori_loop(0, CH // 32, adam, 0)
            for copy in results(k, i):
                copy.start()
        return 0
    lax.fori_loop(0, 2, fifth, 0)

    def drain(i, _):
        for k in range(3):
            c = i * 3 + k

            @pl.when(i < 2)
            def _(k=k, c=c):
                hop(acc, c, r3, c, s3, q3, k, 2).wait_send()
            hop(acc, c, r2, c, s2, q2, k, 1).wait_send()
            hop(acc, 12 + c, r1, 12 + c, s1, q1, k, 0).wait_send()
        return 0
    lax.fori_loop(0, 4, drain, 0)

    def draind(c, _):
        d2d_desc(c).wait_send()
        return 0
    lax.fori_loop(0, 48, draind, 0)

    def written(i, _):
        for k in range(3):
            for copy in results(k, i):
                copy.wait()
        return 0
    lax.fori_loop(0, 2, written, 0)


ANY = pl.BlockSpec(memory_space=pl.ANY)


HBM = pl.BlockSpec(memory_space=pltpu.HBM)
VMEM = pl.BlockSpec(memory_space=pltpu.VMEM)


def reduce_and_update(scal, grads, m, v, w):
    dma = pltpu.SemaphoreType.DMA
    win = jax.ShapeDtypeStruct((WR, 128), F32)
    return pl.pallas_call(
        rs_kernel,
        out_shape=(jax.ShapeDtypeStruct((WR, 128), BF16), win, win, win),
        in_specs=[pl.BlockSpec(memory_space=pltpu.SMEM)] + [HBM] * 9,
        out_specs=[HBM] * 4,
        scratch_shapes=[
            pltpu.VMEM((48 * CH, 128), F32), pltpu.VMEM((24 * CH, 128), F32), pltpu.VMEM((12 * CH, 128), F32),
            pltpu.VMEM((6 * CH, 128), F32), pltpu.VMEM((NST * CH, 128), F32),
            pltpu.VMEM((SHARD,), F32), pltpu.VMEM((WR, 128), BF16),
            dma((48,)), dma((48,)), dma((NST,)), dma((24,)), dma((24,)), dma((12,)), dma((12,)), dma((6,)), dma((6,)),
            dma((2,)), dma((24,)),
        ],
        compiler_params=pltpu.CompilerParams(collective_id=0, has_side_effects=True, vmem_limit_bytes=67043328),
        name="rs",
    )(scal, *grads, m, v, w)


def ag_kernel(wb, m_in, v_in, w_in, flat, out, mt, vt, wt, flat_rows, lsem, isend, irecv, asend, arecv):
    me = my_id()
    delta = deltas(me)
    peers = [coords(me + x) for x in delta]
    load = pltpu.make_async_copy(wb, out.at[pl.ds(pl.multiple_of(me * WR, 32), WR)], lsem.at[0])
    load.start()
    state = ((m_in, mt), (v_in, vt), (w_in, wt))
    loads = [pltpu.make_async_copy(src, dst.at[pl.ds(0, WR)], lsem.at[1 + i]) for i, (src, dst) in enumerate(state)]
    for c in loads:
        c.start()
    entry_barrier(peers)
    load.wait()
    start = me * SHARD
    off = start % 128
    q = (start - off) // 128 - 8 * win_start(me)

    def to_flat_order(src, first):
        def block(row, n, todo):
            for j in range(todo):
                flat_rows[pl.ds(row + j, 8, stride=n), :] = src[pl.ds(pl.multiple_of(row + 8 * j, 8), 8), :]
        each_block(me, block)
        back = (128 - off) % 128
        lane = lax.broadcasted_iota(jnp.int32, (FSTEP, 128), 1)

        def shift(i, _):
            row = pl.multiple_of(i * FSTEP, 8)
            x = pltpu.roll(flat_rows[pl.ds(q + row, FSTEP), :], back, 1)
            y = pltpu.roll(flat_rows[pl.ds(q + row + 1, FSTEP), :], back, 1)
            flat[pl.ds(pl.multiple_of(first + row, 8), FSTEP), :] = jnp.where(lane < 128 - off, x, y)
            return 0
        lax.fori_loop(0, FROWS // FSTEP, shift, 0)

    def slot(k, s, e):
        d1, d2, d3 = COLORS[k]
        w = me + (e % 2) * delta[d1] + (e // 2 % 2) * delta[d2] + (e // 4) * delta[d3]
        return out.at[pl.ds(pl.multiple_of(w * WR + (2 * k + s) * CH, 32), CH)]

    def send(src, dst, k, s, e, step):
        i = (k * 2 + s) * 8 + e + (1 << step)
        return pltpu.make_async_remote_copy(src, dst, isend.at[i], irecv.at[i],
                                            device_id=peers[COLORS[k][step]], device_id_type=MESH)

    def across(src, dst, k, s, e):
        i = (k * 2 + s) * 8 + e
        return pltpu.make_async_remote_copy(src, dst, asend.at[i], arecv.at[i], device_id=peers[0], device_id_type=MESH)

    ks = [(k, s) for s in range(2) for k in range(3)]

    for k, s in ks:
        here = slot(k, s, 0)
        for step in range(3):
            send(here, here, k, s, 0, step).start()
        across(here, here, k, s, 0).start()

    def arrive(e, _):
        for k, s in ks:
            here = slot(k, s, e)
            send(here, here, k, s, e - 1, 0).wait_recv()
            for step in (1, 2):
                @pl.when(e < (1 << step))
                def _(k=k, s=s, here=here, step=step):
                    send(here, here, k, s, e, step).start()
            across(here, here, k, s, e).start()
        return 0

    for i, (lo, hi) in enumerate(((1, 2), (2, 4), (4, 8))):
        loads[i].wait()
        to_flat_order(state[i][1], i * FROWS)
        lax.fori_loop(lo, hi, arrive, 0)

    def finish(i, _):
        any_chunk = out.at[pl.ds(0, CH)]

        def desc(ss, rs):
            return pltpu.make_async_remote_copy(any_chunk, any_chunk, ss.at[i], rs.at[i],
                                                device_id=peers[0], device_id_type=MESH)
        desc(asend, arecv).wait_recv()
        desc(asend, arecv).wait_send()

        @pl.when(i % 8 > 0)
        def _():
            desc(isend, irecv).wait_send()
        return 0
    lax.fori_loop(0, 48, finish, 0)


def all_gather(wb, m, v, w):
    dma = pltpu.SemaphoreType.DMA
    return pl.pallas_call(
        ag_kernel,
        out_shape=(jax.ShapeDtypeStruct((3 * FROWS, 128), F32), jax.ShapeDtypeStruct((NDEV * WR, 128), BF16)),
        in_specs=[HBM] * 4,
        out_specs=[VMEM, ANY],
        scratch_shapes=[pltpu.VMEM((LROWS, 128), F32)] * 4 + [dma((4,)), dma((48,)), dma((48,)), dma((48,)), dma((48,))],
        compiler_params=pltpu.CompilerParams(collective_id=1, has_side_effects=True, vmem_limit_bytes=16 << 20),
        name="ag",
    )(*(pltpu.with_memory_space_constraint(x, pltpu.HBM) for x in (wb, m, v, w)))


BSTART = [block_start(w) for w in range(NDEV)]


def put_kernel(state, slots, m_out, v_out, w_out, o0, o1, o2, o3, o4, o_bqkv, o_b1, o_dvec, tmp, mb, vb, wb, osem):
    outs = (o0, o1, o2, o3, o4)
    stores = []

    def store(src, dst):
        c = pltpu.make_async_copy(src, dst, osem.at[len(stores)])
        c.start()
        stores.append(c)

    def store_tiles(ref, row, lo, hi):
        for k in range(5):
            a, b = max(lo, TOFF[k]), min(hi, TOFF[k + 1])
            if a < b:
                store(ref.at[pl.ds(row + (a - lo) * 8, (b - a) * 8)], outs[k].at[pl.ds((a - TOFF[k]) * 8, (b - a) * 8)])

    for d in range(NDEV):
        t, n, _ = BSTART[d]
        lo = t + n if d else 0
        store_tiles(slots, d * WR + (lo - win_start(d)) * 8, lo, BSTART[d + 1][0] if d + 1 < NDEV else TOFF[6])
    for d in range(1, NDEV):
        t, n, _ = BSTART[d]
        bound = d * SHARD - t * 1024
        p = (lax.broadcasted_iota(jnp.int32, (8, 128), 0) * (n * 128)
             + lax.broadcasted_iota(jnp.int32, (8, 128), 1))
        for j in range(n):
            x = slots[pl.ds(d * WR + (t + j - win_start(d)) * 8, 8), :]
            if j * 128 < bound:
                y = slots[pl.ds((d - 1) * WR + (t + j - win_start(d - 1)) * 8, 8), :]
                x = jnp.where(p + j * 128 < bound, y.astype(F32), x.astype(F32)).astype(BF16)
            tmp[pl.ds(d * 192 + j * 8, 8), :] = x
        store_tiles(tmp, d * 192, t, t + n)
    at = (NDEV - 1) * WR + (TOFF[5] - win_start(NDEV - 1)) * 8
    rows = slots[pl.ds(at, 96), :].astype(F32)
    for j in range(24):
        o_bqkv[:, j * 128:(j + 1) * 128] = rows[j:j + 1].astype(BF16)
    for j in range(22):
        o_b1[:, j * 128:(j + 1) * 128] = rows[24 + j:25 + j].astype(BF16)
    for i in range(6):
        for j in range(8):
            o_dvec[0, i:i + 1, j * 128:(j + 1) * 128] = rows[46 + 8 * i + j:47 + 8 * i + j].astype(BF16)
    for i, (buf, out) in enumerate(((mb, m_out), (vb, v_out), (wb, w_out))):
        def cut(row, rows, cols, e, i=i, buf=buf):
            buf[pl.ds(e, rows * cols)] = state[pl.ds(i * FROWS + row, rows), :][:, :cols].reshape(rows * cols)
        pieces(cut)
        store(buf, out)
    for c in stores:
        c.wait()


def put(state, slots):
    flat = jax.ShapeDtypeStruct((SHARD,), F32)
    return pl.pallas_call(
        put_kernel,
        out_shape=(flat,) * 3 + tuple(jax.ShapeDtypeStruct(((TOFF[k + 1] - TOFF[k]) * 8, 128), BF16) for k in range(5)) + (
            jax.ShapeDtypeStruct((1, SMALL[0]), BF16), jax.ShapeDtypeStruct((1, SMALL[1]), BF16),
            jax.ShapeDtypeStruct((1, 6, 1024), BF16)),
        in_specs=[VMEM] * 2,
        out_specs=[HBM] * 8 + [VMEM] * 3,
        scratch_shapes=[pltpu.VMEM((NDEV * 192, 128), BF16)] + [pltpu.VMEM((SHARD,), F32)] * 3 + [
            pltpu.SemaphoreType.DMA((48,))],
        compiler_params=pltpu.CompilerParams(vmem_limit_bytes=16 << 20),
        name="put",
    )(state, slots)


def to_tiles(x):
    r, c = x.shape
    return x.reshape(r // 8, 8, c // 128, 128).transpose(0, 2, 1, 3).reshape(r * c // 128, 128)


def from_tiles(x, r, c):
    return x.reshape(r // 8, c // 128, 8, 128).transpose(0, 2, 1, 3).reshape(r, c)


def solution(mesh):
    def body(g_emb, g_qkv, g_o, g_w1, g_w2, g_bqkv, g_b1, g_dvec, m, v, w, lr, beta1, beta2, eps, step):
        big = [to_tiles(x.reshape(rc)) for x, rc in zip((g_emb, g_qkv, g_o, g_w1, g_w2), BIG)]
        small = jnp.concatenate([g_bqkv.reshape(-1, 128), g_b1.reshape(-1, 128), g_dvec.reshape(-1, 128),
                                 jnp.zeros((SMALL_TILES * 8 - sum(SMALL) // 128, 128), F32)])
        t = step.astype(F32)
        scal = jnp.stack([lr, beta1, beta2, eps, 1.0 / (1.0 - beta1 ** t), 1.0 / (1.0 - beta2 ** t)])
        m_new, v_new, w_new, *outs = put(*all_gather(*reduce_and_update(scal, (*big, small), m, v, w)))
        wbs = [from_tiles(o, *rc) for o, rc in zip(outs, BIG)]
        return (m_new, v_new, w_new, wbs[0], wbs[1][None], wbs[2][None], wbs[3][None], wbs[4][None], *outs[5:])

    g3 = P(AXES, None, None)
    g4 = P(AXES, None, None, None)
    flat = P(AXES)
    rep = P()
    in_specs = (g3, g4, g4, g4, g4, g3, g3, g4, flat, flat, flat, rep, rep, rep, rep, rep)
    out_specs = (flat, flat, flat, rep, rep, rep, rep, rep, rep, rep, rep)
    return jax.shard_map(body, mesh=mesh, in_specs=in_specs, out_specs=out_specs, check_vma=False)
```
